32 devices in a mesh: gx: 8 (over y, x, core), gy: 4 (over z).
Axes of the slice: x: 2, y: 2, z: 4, core: 2. Of those that a mesh axis runs over, the one named last changes fastest.
Arguments:
- object_field: float32 [2, 256, 512], P(None, 'gy', 'gx'), may hold values from -1 to 1
- probe_modes: float32 [2, 1024, 128], P(None, ('gy', 'gx')), may hold values from -1.5 to 1.5
- positions: int32 [4, 8, 12, 2], P('gy', 'gx'), may hold values from 4 to 60, as said below
- amplitudes: float32 [4, 8, 12, 128, 128], P('gy', 'gx'), may hold values from 0 to 2
Outputs:
- object_out: float32 [2, 256, 512], P(None, 'gy', 'gx')
- probe_out: float32 [2, 1024, 128], P(None, ('gy', 'gx'))
The draws below stay inside these ranges and needn't reach their ends.
Inputs may be any that keep to these rules, and one draw needn't show every extreme that they name: `positions`: each entry is a (row, column) inside its own tile; the centres of one tile lie at distinct cells of the 16 grid, each moved from the cell's middle by at most 4 cells along each dimension.
All inputs are finite; a program needn't handle non-finite values.
Results may differ from the reference program's by a relative error of at most 0.00065.
The reference program's roundings to bfloat16 on the way count: a program that leaves them out, or rounds other values in their place, can miss the bound.
Values sent between devices are 32-bit elements; how exact they have to be, the bound alone decides.
A program may use at most 64 MiB of HBM per device.

```python
import math
import jax
import jax.numpy as jnp
from jax import lax

PROBE = 128
MODES = 8
TILE = 64
STRIDE = 16
POS_DEV = 12
ITERS = 2
TILES_Y = 4
TILES_X = 8
NY = 256
NX = 512


def draw_positions(key, part):
    grid_cells = TILE // STRIDE
    tile_count = TILES_Y * TILES_X
    keys = jax.random.split(jax.random.fold_in(key, 11), tile_count)

    def one_tile(subkey):
        chosen = jax.random.permutation(subkey, grid_cells * grid_cells)[:POS_DEV]
        jitter = jax.random.randint(jax.random.fold_in(subkey, 3), (POS_DEV, 2), -4, 5)
        cells = jnp.stack([chosen // grid_cells, chosen % grid_cells], axis=1)
        return cells * STRIDE + STRIDE // 2 + jitter
    return jax.vmap(one_tile)(keys).reshape(TILES_Y, TILES_X, POS_DEV, 2).astype(jnp.int32)


def draw_object_field(key, part):
    base = jax.random.fold_in(key, 23)
    magnitude_key = jax.random.fold_in(base, 1)
    phase_key = jax.random.fold_in(base, 2)
    magnitude = jax.random.uniform(magnitude_key, (NY, NX), jnp.float32, 0.5, 1.0)
    phase = jax.random.uniform(phase_key, (NY, NX), jnp.float32, -0.6, 0.6)
    return jnp.stack([magnitude * jnp.cos(phase), magnitude * jnp.sin(phase)]).astype(jnp.float32)


def steps_of(stream_key, dims, shards, least, high):
    level = 1.0
    for position, blocks in shards:
        heights = jax.random.uniform(jax.random.fold_in(jax.random.fold_in(stream_key, 6), position), (blocks,), jnp.float32, least / len(shards), high / len(shards))
        level = level * jnp.repeat(jnp.exp(heights), dims[position] // blocks).reshape((-1,) + (1,) * (len(dims) - 1 - position))
    return level


def normal_values(rng, dims, deviation, bound, shards=(), kind=jnp.bfloat16):
    values = jax.random.normal(rng, dims, jnp.float32) * deviation
    if len(shards) > 0:
        values = steps_of(rng, dims, shards, -0.22, 0.18) * values
    return jnp.clip(values, min=-bound, max=bound).astype(kind)


def setup_inputs(seed: int = 0) -> dict:
    streams_of = jax.random.split(jax.random.key(seed), 5)
    return {
        "object_field": draw_object_field(jax.random.fold_in(streams_of[4], 71), 0),
        "probe_modes": normal_values(streams_of[1], (2, MODES * PROBE, PROBE), 0.25, 1.5, ((1, 32),), jnp.float32),
        "positions": draw_positions(jax.random.fold_in(streams_of[4], 71), 0),
        "amplitudes": jnp.clip(2.0 * jax.random.uniform(streams_of[3], (TILES_Y, TILES_X, POS_DEV, PROBE, PROBE), jnp.float32) ** steps_of(streams_of[3], (TILES_Y, TILES_X, POS_DEV, PROBE, PROBE), ((0, 4), (1, 8)), -0.2, 0.2), 0.0, 2.0),
    }


SOFT_FLOOR = 0.05
OBJECT_REG = 1.0
PROBE_REG = 1.0

def tables(probe_side, sign_flip):
    indices = jnp.arange(probe_side, dtype=jnp.int32)
    phases = indices[:, None] * indices[None, :] % probe_side
    angles = phases.astype(jnp.float32) * (2.0 * math.pi / probe_side)
    factor = 1.0 / math.sqrt(probe_side)
    cosine = jnp.cos(angles) * factor
    sine_part = sign_flip * jnp.sin(angles) * factor
    left_op = jnp.stack([jnp.stack([cosine, -sine_part]), jnp.stack([sine_part, cosine])]).transpose(0, 2, 1, 3)
    right_op = jnp.stack([jnp.stack([cosine, sine_part]), jnp.stack([-sine_part, cosine])]).transpose(0, 2, 1, 3)
    return (left_op.astype(jnp.bfloat16), right_op.astype(jnp.bfloat16))

def transform(signal, operators):
    left_op, right_op = operators
    signal = lax.optimization_barrier(signal)
    halfway = jnp.einsum('dpcr,crmq->dpmq', left_op.astype(jnp.float32), signal.astype(jnp.float32), precision=lax.Precision.HIGHEST).astype(jnp.bfloat16)
    halfway = lax.optimization_barrier(halfway)
    return jnp.einsum('crmq,cqdk->drmk', halfway.astype(jnp.float32), right_op.astype(jnp.float32), precision=lax.Precision.HIGHEST)

def position_terms(patch_obj, probe, measured, forward, inverse):
    obj_real = patch_obj[0][:, None, :]
    obj_imag = patch_obj[1][:, None, :]
    wave_real = probe[0] * obj_real - probe[1] * obj_imag
    wave_imag = probe[0] * obj_imag + probe[1] * obj_real
    signal = jnp.stack([wave_real, wave_imag]).astype(jnp.bfloat16)
    spectrum = transform(signal, forward)
    intensity = lax.optimization_barrier(jnp.sum(spectrum[0] * spectrum[0] + spectrum[1] * spectrum[1], axis=1))
    shrink = 1.0 - measured / jnp.sqrt(intensity + SOFT_FLOOR)
    residual = (spectrum * shrink[None, :, None, :]).astype(jnp.bfloat16)
    change = transform(residual, inverse)
    grad_real = lax.optimization_barrier(jnp.sum(probe[0] * change[0] + probe[1] * change[1], axis=1))
    grad_imag = lax.optimization_barrier(jnp.sum(probe[0] * change[1] - probe[1] * change[0], axis=1))
    probe_real = obj_real * change[0] + obj_imag * change[1]
    probe_imag = obj_real * change[1] - obj_imag * change[0]
    weight_probe = patch_obj[0] * patch_obj[0] + patch_obj[1] * patch_obj[1]
    return (jnp.stack([grad_real, grad_imag]), jnp.stack([probe_real, probe_imag]), weight_probe)

def reference(object_field, probe_modes, positions, amplitudes):
    margin = PROBE // 2
    forward = tables(PROBE, -1.0)
    inverse = tables(PROBE, 1.0)
    tile_rows = jnp.arange(TILES_Y, dtype=jnp.int32)[:, None, None] * TILE
    tile_cols = jnp.arange(TILES_X, dtype=jnp.int32)[None, :, None] * TILE
    row_list = (positions[..., 0] + tile_rows).reshape(-1).astype(jnp.int32)
    col_list = (positions[..., 1] + tile_cols).reshape(-1).astype(jnp.int32)
    measured_all = amplitudes.reshape(-1, PROBE, PROBE)
    probe = probe_modes.reshape(2, MODES, PROBE, PROBE).transpose(0, 2, 1, 3)
    current = object_field
    for iteration in range(ITERS):
        padded = jnp.pad(current, ((0, 0), (margin, margin), (margin, margin)))
        weight_obj = lax.optimization_barrier(jnp.sum(probe[0] * probe[0] + probe[1] * probe[1], axis=1))

        def visit(running, visit_item):
            grad_obj, grad_probe, weight_probe = running
            row_at, col_at, measured = visit_item
            zero_index = jnp.int32(0)
            patch_obj = lax.dynamic_slice(padded, (zero_index, row_at, col_at), (2, PROBE, PROBE))
            g_obj, g_probe, w_probe = position_terms(patch_obj, probe, measured, forward, inverse)
            stacked = jnp.concatenate([g_obj, weight_obj[None]], axis=0)
            before = lax.dynamic_slice(grad_obj, (zero_index, row_at, col_at), (3, PROBE, PROBE))
            grad_obj = lax.dynamic_update_slice(grad_obj, before + stacked, (zero_index, row_at, col_at))
            return ((grad_obj, grad_probe + g_probe, weight_probe + w_probe), None)
        initial = (jnp.zeros((3, NY + PROBE, NX + PROBE), jnp.float32), jnp.zeros((2, PROBE, MODES, PROBE), jnp.float32), jnp.zeros((PROBE, PROBE), jnp.float32))
        (grad_obj, grad_probe, weight_probe), _ = lax.scan(visit, initial, (row_list, col_list, measured_all))
        inner = grad_obj[:, margin:margin + NY, margin:margin + NX]
        new_object = current - inner[0:2] / (inner[2] + OBJECT_REG)
        probe = probe - grad_probe / (weight_probe[:, None, :] + PROBE_REG)
        current = new_object
    return (current, probe.transpose(0, 2, 1, 3).reshape(2, MODES * PROBE, PROBE))
```

```python
import functools
import math
from types import SimpleNamespace

import jax
import jax.numpy as jnp
import numpy as np
from jax import lax
from jax.experimental import pallas as pl
from jax.experimental.pallas import tpu as pltpu
from jax.sharding import PartitionSpec as P

ITERS = 2
SOFT_FLOOR = 0.05
OBJECT_REG = 1.0
PROBE_REG = 1.0
CHUNK = 16
MESH = pl.DeviceIdType.MESH
F32 = jnp.float32
BF16 = jnp.bfloat16


class Plan:
    def __init__(self, mesh, object_field, probe_modes, positions, amplitudes):
        self.gx, self.gy = mesh.shape["gx"], mesh.shape["gy"]
        self.side = amplitudes.shape[-1]
        self.count = amplitudes.shape[-3]
        self.tile = object_field.shape[1] // self.gy
        self.rows = probe_modes.shape[1]
        self.modes = self.rows // self.side
        self.own = self.rows // (self.gx * self.gy)
        self.chips = self.gx // 2
        self.split = self.own >= 8
        self.cores = 2 if self.split else 1
        self.piece = self.own if self.split else 2 * self.own
        self.block = self.rows // self.gy
        self.steps = min(self.modes, self.gy)
        self.step_modes = self.modes // self.steps
        self.step_blocks = self.gy // self.steps
        self.weights = max(1, self.side // self.block)
        self.weight_rows = self.weights * self.block
        self.quads = self.count // 4
        self.step_bodies = self.step_modes * self.quads
        assert self.tile * 2 == self.side and self.count % 4 == 0
        assert self.piece % 8 == 0 and self.gx % 2 == 0

    def scratch(self):
        s, n = self.side, self.count
        sems = pltpu.SemaphoreType.DMA
        k, c, g = self.piece, self.chips, self.gy
        vmem = pltpu.VMEM
        return dict(
            amp=vmem((n, s, s), F32),
            fwd=vmem((2 * s, 2 * s), BF16),
            inv=vmem((2 * s, 2 * s), BF16),
            probe=vmem((ITERS, 2, self.rows, s), F32),
            patch=vmem((n, 2, s, s), F32),
            ext=vmem((4, 3 * self.tile, s), F32),
            far=vmem((self.modes, n, s, 2 * s), F32),
            shrink=vmem((n, s, s), F32),
            delta=vmem((self.modes, n, s, 2 * s), F32),
            ops0=vmem((2 * s, 4 * s), BF16),
            ops1=vmem((2 * s, 4 * s), BF16),
            ops2=vmem((2 * s, 4 * s), BF16),
            mids0=vmem((4 * s, 2 * s), BF16),
            mids1=vmem((4 * s, 2 * s), BF16),
            mids2=vmem((4 * s, 2 * s), BF16),
            spread=vmem((n, 2, 2 * s, s), F32),
            weight=vmem((2 * s, s), F32),
            grad=vmem((ITERS, 2, self.rows, s), F32),
            wgrad=vmem((ITERS, 1, self.weight_rows, s), F32),
            obj=vmem((ITERS, self.tile, s), F32),
            halo=vmem((ITERS, 8, self.tile, s), F32),
            fold_tx=vmem((ITERS, 3, 3 * self.tile, s), F32),
            fold_rx=vmem((ITERS, 8, self.tile, s), F32),
            wfold_tx=vmem((ITERS, 3, 3 * self.tile, s), F32),
            wfold_rx=vmem((ITERS, 8, self.tile, s), F32),
            rx_a=vmem((ITERS, g, c, 2, k, s), F32),
            sum_a=vmem((ITERS, g, c, 2, k, s), F32),
            rx_b=vmem((ITERS, g, c - 1, 2, k, s), F32),
            sum_b=vmem((ITERS, g, 2, k, s), F32),
            rx_c=vmem((ITERS, g - 1, 2, k, s), F32),
            wrx_a=vmem((ITERS, self.weights, c, 1, k, s), F32),
            wsum_a=vmem((ITERS, self.weights, c, 1, k, s), F32),
            wrx_b=vmem((ITERS, self.weights, c - 1, 1, k, s), F32),
            wsum_b=vmem((ITERS, self.weights, 1, k, s), F32),
            wrx_c=vmem((ITERS, self.weights, g - 1, 1, k, s), F32),
            wsum=vmem((ITERS, self.weights, k, s), F32),
            load_sem=sems((3,)),
            a_sem=sems((2, ITERS, g)),
            b_sem=sems((2, ITERS, g)),
            c_sem=sems((2, ITERS, g)),
            wa_sem=sems((2, ITERS, self.weights)),
            wb_sem=sems((2, ITERS, self.weights)),
            wc_sem=sems((2, ITERS, self.weights)),
            row_sem=sems((ITERS, 1 + g)),
            gb_sem=sems((2, ITERS, g)),
            ga_sem=sems((2, ITERS, g)),
            halo_sem=sems((2, ITERS, 8)),
            fold_sem=sems((2, ITERS, 8)),
            wfold_sem=sems((2, ITERS, 8)),
        )


def aligned(value):
    return pl.multiple_of(value, 8)


def program(plan, names, places, object_ref, own_ref, amp_hbm, fwd_hbm, inv_hbm, object_out, probe_out, *scratch):
    r = SimpleNamespace(**dict(zip(names, scratch)))
    side, tile, piece, chips = plan.side, plan.tile, plan.piece, plan.chips
    nx, ny = plan.gx, plan.gy
    gx, gy = lax.axis_index("gx"), lax.axis_index("gy")
    chip, core = lax.div(gx, 2), lax.rem(gx, 2)
    lane = lax.broadcasted_iota(jnp.int32, (1, side), 1)
    low = lane < tile

    def half_turn(value):
        return pltpu.roll(value, tile, 1)

    def device(x, y):
        return {"gx": x, "gy": y}

    mate = device(gx + 1 - 2 * core, gy)
    chip_peers = [device(lax.rem(chip + d, chips) * 2 + core, gy) for d in range(1, chips)]
    row_peers = [device(gx, lax.rem(gy + d, ny)) for d in range(1, ny)]
    offsets = [(dy, dx) for dy in (-1, 0, 1) for dx in (-1, 0, 1) if (dy, dx) != (0, 0)]

    def inside(dy, dx):
        ok = gx >= 0
        if dy < 0:
            ok &= gy > 0
        if dy > 0:
            ok &= gy < ny - 1
        if dx < 0:
            ok &= gx > 0
        if dx > 0:
            ok &= gx < nx - 1
        return ok

    def send(source, target, sems, who):
        pltpu.make_async_remote_copy(
            src_ref=source, dst_ref=target, send_sem=sems[0], recv_sem=sems[1], device_id=who, device_id_type=MESH
        ).start()

    def await_bytes(ref, sem):
        pltpu.make_async_copy(ref, ref, sem).wait()

    loads = [
        pltpu.make_async_copy(amp_hbm, r.amp, r.load_sem.at[0]),
        pltpu.make_async_copy(fwd_hbm, r.fwd, r.load_sem.at[1]),
        pltpu.make_async_copy(inv_hbm, r.inv, r.load_sem.at[2]),
    ]
    for copy in loads:
        copy.start()

    for ref in (r.halo, r.fold_rx, r.wfold_rx):
        ref[...] = jnp.zeros(ref.shape, F32)

    def signal(who):
        pl.semaphore_signal(pltpu.get_barrier_semaphore(), inc=1, device_id=who, device_id_type=MESH)

    r.obj[0] = jnp.concatenate([object_ref[0], object_ref[1]], axis=1)
    home = lax.mul(lax.mul(gy, chips) + chip, plan.cores * piece) + (core * piece if plan.split else 0)
    for plane in range(2):
        r.probe[0, plane, pl.ds(aligned(home), piece), :] = own_ref[plane]

    greetings = 1 + (chips - 1) + (ny - 1)
    for who in [mate] + chip_peers + row_peers:
        signal(who)
    expected = greetings
    for dy, dx in offsets:
        ok = inside(dy, dx)
        expected = expected + ok.astype(jnp.int32)

        @pl.when(ok)
        def _():
            signal(device(gx + dx, gy + dy))

    r.grad[...] = jnp.zeros(r.grad.shape, F32)
    rim = jnp.zeros((tile, side), F32)
    r.weight[:tile] = rim
    r.weight[tile + side :] = rim

    def rims(j, carry):
        for plane in range(2):
            r.spread[j, plane, :tile] = rim
            r.spread[j, plane, tile + side :] = rim
        return carry

    lax.fori_loop(0, plan.count, rims, 0)
    pl.semaphore_wait(pltpu.get_barrier_semaphore(), expected)

    def to_neighbours(it, sources, target, sems):
        for n, (dy, dx) in enumerate(offsets):

            @pl.when(inside(dy, dx))
            def _():
                send(sources(dy, dx), target.at[it, n], (sems.at[0, it, n], sems.at[1, it, n]), device(gx + dx, gy + dy))

    def from_neighbours(it, target, sems):
        for n, (dy, dx) in enumerate(offsets):

            @pl.when(inside(-dy, -dx))
            def _():
                await_bytes(target.at[it, n], sems.at[1, it, n])

    def sent_to_neighbours(it, target, sems):
        for n, (dy, dx) in enumerate(offsets):

            @pl.when(inside(dy, dx))
            def _():
                await_bytes(target.at[it, n], sems.at[0, it, n])

    def rows_of(block, at_chip, at_core):
        start = (block * chips + at_chip) * (plan.cores * piece)
        return pl.ds(aligned(start + at_core * piece), piece)

    def my_core():
        return core if plan.split else 0

    def probe_piece(it, block):
        return r.probe.at[it, :, rows_of(block, chip, my_core())]

    def probe_span(it, pieces):
        return r.probe.at[it, :, pl.ds(0, pieces * piece)]

    def spread_chips(it, block):
        for who in chip_peers:
            send(probe_piece(it, block), probe_piece(it, block), (r.gb_sem.at[0, it, block], r.gb_sem.at[1, it, block]), who)

    def got_chips(it, block):
        await_bytes(probe_span(it, chips - 1), r.gb_sem.at[1, it, block])

    def spread_cores(it, block):
        if plan.split:
            for q in range(chips):
                view = r.probe.at[it, :, rows_of(block, q, core)]
                send(view, view, (r.ga_sem.at[0, it, block], r.ga_sem.at[1, it, block]), mate)

    def got_cores(it, block):
        if plan.split:
            await_bytes(probe_span(it, chips), r.ga_sem.at[1, it, block])

    def first_order(t):
        value, bit = 0, 1
        group = lax.div(gy, plan.step_blocks)
        while bit < plan.steps:
            value = value + bit * lax.rem(lax.div(group, bit) + lax.div(t, bit), 2)
            bit *= 2
        return value

    def blocks_of(step):
        return [step * plan.step_blocks + i for i in range(plan.step_blocks)]

    grads = SimpleNamespace(
        terms=r.grad,
        rx_a=r.rx_a,
        sum_a=r.sum_a,
        rx_b=r.rx_b,
        sum_b=r.sum_b,
        rx_c=r.rx_c,
        a_sem=r.a_sem,
        b_sem=r.b_sem,
        c_sem=r.c_sem,
    )
    weights = SimpleNamespace(
        terms=r.wgrad,
        rx_a=r.wrx_a,
        sum_a=r.wsum_a,
        rx_b=r.wrx_b,
        sum_b=r.wsum_b,
        rx_c=r.wrx_c,
        a_sem=r.wa_sem,
        b_sem=r.wb_sem,
        c_sem=r.wc_sem,
    )

    def reduce_a(ch, it, b):
        for q in range(chips):
            at_core = (1 - core) if plan.split else 0
            send(
                ch.terms.at[it, :, rows_of(b, q, at_core)],
                ch.rx_a.at[it, b, q],
                (ch.a_sem.at[0, it, b], ch.a_sem.at[1, it, b]),
                mate,
            )

    def reduce_b(ch, it, b):
        await_bytes(ch.rx_a.at[it, b], ch.a_sem.at[1, it, b])
        for q in range(chips):
            ch.sum_a[it, b, q] = ch.terms[it, :, rows_of(b, q, my_core()), :] + ch.rx_a[it, b, q]
        for d, who in enumerate(chip_peers):
            send(
                ch.sum_a.at[it, b, lax.rem(chip + d + 1, chips)],
                ch.rx_b.at[it, b, d],
                (ch.b_sem.at[0, it, b], ch.b_sem.at[1, it, b]),
                who,
            )

    def reduced_b(ch, it, b):
        await_bytes(ch.rx_b.at[it, b], ch.b_sem.at[1, it, b])
        total = ch.sum_a[it, b, chip]
        for d in range(chips - 1):
            total = total + ch.rx_b[it, b, d]
        ch.sum_b[it, b] = total

    def reduce_weights(it, w):
        reduced_b(weights, it, w)
        for d, who in enumerate(row_peers):
            send(
                weights.sum_b.at[it, w],
                weights.rx_c.at[it, w, d],
                (weights.c_sem.at[0, it, w], weights.c_sem.at[1, it, w]),
                who,
            )

    def settle_weights(it):
        for w in range(plan.weights):
            await_bytes(weights.rx_c.at[it, w], weights.c_sem.at[1, it, w])
            total = weights.sum_b[it, w]
            for d in range(ny - 1):
                total = total + weights.rx_c[it, w, d]
            r.wsum[it, w] = total[0] + PROBE_REG

    def to_owner(it, b):
        reduced_b(grads, it, b)

        @pl.when(gy != b)
        def _():
            slot = lax.rem(gy - b - 1 + ny, ny)
            send(
                grads.sum_b.at[it, b],
                grads.rx_c.at[it, slot],
                (grads.c_sem.at[0, it, b], grads.c_sem.at[1, it, 0]),
                device(gx, b),
            )

    def owned(it, b):
        await_bytes(grads.rx_c.at[it], grads.c_sem.at[1, it, 0])
        change = grads.sum_b[it, b]
        for d in range(ny - 1):
            change = change + grads.rx_c[it, d]
        place = rows_of(b, chip, my_core())
        down = r.wsum[it, lax.rem(b, plan.weights)]
        return [r.probe[it, plane, place, :] - change[plane] / down for plane in range(2)]

    def spread_rows(it, b):
        for who in row_peers:
            send(probe_piece(it, b), probe_piece(it, b), (r.row_sem.at[it, ny], r.row_sem.at[it, b]), who)

    def renew(b):
        @pl.when(gy == b)
        def _():
            new = owned(0, b)
            for plane in range(2):
                r.probe[1, plane, rows_of(b, chip, my_core()), :] = new[plane]
            spread_rows(1, b)
            spread_chips(1, b)

    def pass_chips(it, b):
        @pl.when(gy != b)
        def _():
            await_bytes(probe_piece(it, b), r.row_sem.at[it, b])
            spread_chips(it, b)

    def pass_cores(it, b):
        got_chips(it, b)
        spread_cores(it, b)

    grads = SimpleNamespace(
        terms=r.grad,
        rx_a=r.rx_a,
        sum_a=r.sum_a,
        rx_b=r.rx_b,
        sum_b=r.sum_b,
        rx_c=r.rx_c,
        a_sem=r.a_sem,
        b_sem=r.b_sem,
        c_sem=r.c_sem,
    )
    weights = SimpleNamespace(
        terms=r.wgrad,
        rx_a=r.wrx_a,
        sum_a=r.wsum_a,
        rx_b=r.wrx_b,
        sum_b=r.wsum_b,
        rx_c=r.wrx_c,
        a_sem=r.wa_sem,
        b_sem=r.wb_sem,
        c_sem=r.wc_sem,
    )

    def reduce_a(ch, it, b):
        for q in range(chips):
            at_core = (1 - core) if plan.split else 0
            send(
                ch.terms.at[it, :, rows_of(b, q, at_core)],
                ch.rx_a.at[it, b, q],
                (ch.a_sem.at[0, it, b], ch.a_sem.at[1, it, b]),
                mate,
            )

    def reduce_b(ch, it, b):
        await_bytes(ch.rx_a.at[it, b], ch.a_sem.at[1, it, b])
        for q in range(chips):
            ch.sum_a[it, b, q] = ch.terms[it, :, rows_of(b, q, my_core()), :] + ch.rx_a[it, b, q]
        for d, who in enumerate(chip_peers):
            send(
                ch.sum_a.at[it, b, lax.rem(chip + d + 1, chips)],
                ch.rx_b.at[it, b, d],
                (ch.b_sem.at[0, it, b], ch.b_sem.at[1, it, b]),
                who,
            )

    def reduced_b(ch, it, b):
        await_bytes(ch.rx_b.at[it, b], ch.b_sem.at[1, it, b])
        total = ch.sum_a[it, b, chip]
        for d in range(chips - 1):
            total = total + ch.rx_b[it, b, d]
        ch.sum_b[it, b] = total

    def reduce_weights(it, w):
        reduced_b(weights, it, w)
        for d, who in enumerate(row_peers):
            send(
                weights.sum_b.at[it, w],
                weights.rx_c.at[it, w, d],
                (weights.c_sem.at[0, it, w], weights.c_sem.at[1, it, w]),
                who,
            )

    def settle_weights(it):
        for w in range(plan.weights):
            await_bytes(weights.rx_c.at[it, w], weights.c_sem.at[1, it, w])
            total = weights.sum_b[it, w]
            for d in range(ny - 1):
                total = total + weights.rx_c[it, w, d]
            r.wsum[it, w] = total[0] + PROBE_REG

    def to_owner(it, b):
        reduced_b(grads, it, b)

        @pl.when(gy != b)
        def _():
            slot = lax.rem(gy - b - 1 + ny, ny)
            send(
                grads.sum_b.at[it, b],
                grads.rx_c.at[it, slot],
                (grads.c_sem.at[0, it, b], grads.c_sem.at[1, it, 0]),
                device(gx, b),
            )

    def owned(it, b):
        await_bytes(grads.rx_c.at[it], grads.c_sem.at[1, it, 0])
        change = grads.sum_b[it, b]
        for d in range(ny - 1):
            change = change + grads.rx_c[it, d]
        place = rows_of(b, chip, my_core())
        down = r.wsum[it, lax.rem(b, plan.weights)]
        return [r.probe[it, plane, place, :] - change[plane] / down for plane in range(2)]

    def spread_rows(it, b):
        for who in row_peers:
            send(probe_piece(it, b), probe_piece(it, b), (r.row_sem.at[it, ny], r.row_sem.at[it, b]), who)

    def renew(b):
        @pl.when(gy == b)
        def _():
            new = owned(0, b)
            for plane in range(2):
                r.probe[1, plane, rows_of(b, chip, my_core()), :] = new[plane]
            spread_rows(1, b)
            spread_chips(1, b)

    def pass_chips(it, b):
        @pl.when(gy != b)
        def _():
            await_bytes(probe_piece(it, b), r.row_sem.at[it, b])
            spread_chips(it, b)

    def pass_cores(it, b):
        got_chips(it, b)
        spread_cores(it, b)

    def over(step, act, *rest):
        if 0 <= step < plan.steps:
            for b in blocks_of(step):
                act(*rest, b)

    def widen(it):
        halo = {o: (lambda n: lambda: r.halo[it, n])(n) for n, o in enumerate(offsets)}
        for dy in (-1, 0, 1):
            left = halo[(-dy, 1)]()
            right = halo[(-dy, -1)]()
            centre = r.obj[it] if dy == 0 else halo[(-dy, 0)]()
            band = slice((dy + 1) * tile, (dy + 2) * tile)
            r.ext[0, band] = jnp.where(low, left, half_turn(centre))
            r.ext[1, band] = right
            r.ext[2, band] = jnp.where(low, half_turn(left), centre)
            r.ext[3, band] = half_turn(right)

    def cut_patches(it):
        def one(j, total):
            window = pl.ds(places[j, 0], side)
            col = places[j, 1]
            turn = lax.rem(side - col, side)
            for plane in range(2):
                one_half = pltpu.roll(r.ext[2 * plane, window, :], turn, 1)
                other = pltpu.roll(r.ext[2 * plane + 1, window, :], turn, 1)
                part = jnp.where(lane < side - col, one_half, other)
                r.patch[j, plane] = part
                total = total + part * part
            r.shrink[j] = jnp.zeros((side, side), F32)
            return total

        def some(i, total):
            for n in range(2):
                total = one(2 * i + n, total)
            return total

        total = lax.fori_loop(0, plan.count // 2, some, jnp.zeros((side, side), F32))
        for w in range(plan.weight_rows // side):
            r.wgrad[it, 0, w * side : (w + 1) * side, :] = total

    def sow(load, planes):
        lefts = [0.0] * planes
        rights = [0.0] * planes
        for j in range(plan.count):
            col = places[j, 1]
            for plane in range(planes):
                turned = pltpu.roll(load(j, plane), col, 1)
                lefts[plane] = lefts[plane] + jnp.where(lane >= col, turned, 0.0)
                rights[plane] = rights[plane] + jnp.where(lane < col, turned, 0.0)
        return (
            jnp.where(low, lefts[0], half_turn(lefts[-1])),
            jnp.where(low, half_turn(lefts[0]), lefts[-1]),
            jnp.where(low, rights[0], half_turn(rights[-1])),
        )

    band = tile

    def gather_rows(i, source):
        def load(j, plane):
            return source(j, plane, pl.ds(tile + i * band - places[j, 0], band))

        return load

    def fold_weights(it):
        total = jnp.zeros((side, side), F32)
        for m in range(plan.modes):
            for plane in range(2):
                part = r.probe[it, plane, m * side : (m + 1) * side, :]
                total = total + part * part
        r.weight[tile : tile + side] = total

        def rows_at(i, carry):
            tiles = sow(gather_rows(i, lambda j, plane, at: r.weight[at, :]), 1)
            for n in range(3):
                r.wfold_tx[it, n, pl.ds(aligned(i * band), band), :] = tiles[n]
            return carry

        lax.fori_loop(0, 3 * tile // band, rows_at, 0)
        to_neighbours(it, lambda dy, dx: r.wfold_tx.at[it, dx + 1, pl.ds((dy + 1) * tile, tile)], r.wfold_rx, r.wfold_sem)

    def fold_object(it):
        def rows_at(i, carry):
            tiles = sow(gather_rows(i, lambda j, plane, at: r.spread[j, plane, at, :]), 2)
            for n in range(3):
                r.fold_tx[it, n, pl.ds(aligned(i * band), band), :] = tiles[n]
            return carry

        lax.fori_loop(0, 3 * tile // band, rows_at, 0)
        to_neighbours(it, lambda dy, dx: r.fold_tx.at[it, dx + 1, pl.ds((dy + 1) * tile, tile)], r.fold_rx, r.fold_sem)

    def new_object(it):
        from_neighbours(it, r.wfold_rx, r.wfold_sem)
        from_neighbours(it, r.fold_rx, r.fold_sem)
        change = r.fold_tx[it, 1, tile : 2 * tile]
        down = r.wfold_tx[it, 1, tile : 2 * tile] + OBJECT_REG
        for n in range(8):
            change = change + r.fold_rx[it, n]
            down = down + r.wfold_rx[it, n]
        return r.obj[it] - change / down

    def send_object(it):
        to_neighbours(it, lambda dy, dx: r.obj.at[it], r.halo, r.halo_sem)

    def dot(left, right):
        return jnp.dot(left, right, preferred_element_type=F32)

    def quad(k, order):
        step = lax.div(k, plan.step_bodies)
        within = lax.rem(k, plan.step_bodies)
        return order(step) * plan.step_modes + lax.div(within, plan.quads), 4 * lax.rem(within, plan.quads)

    def half_way(operator, ops, mids):
        for h in range(2):
            half = dot(operator[...], ops[:, h * 2 * side : (h + 1) * 2 * side])
            for s in range(2):
                cols = slice(s * side, (s + 1) * side)
                target = slice((2 * h + s) * side, (2 * h + s + 1) * side)
                mids[target, :side] = half[:side, cols].astype(BF16)
                mids[target, side:] = half[side:, cols].astype(BF16)

    def chunk_rows(m, q):
        return pl.ds(pl.multiple_of(m * side + q * CHUNK, CHUNK), CHUNK)

    def waves(it, k, order, ops):
        m, j = quad(k, order)
        for q in range(side // CHUNK):
            upper = slice(q * CHUNK, (q + 1) * CHUNK)
            lower = slice(side + q * CHUNK, side + (q + 1) * CHUNK)
            p_re = r.probe[it, 0, chunk_rows(m, q), :]
            p_im = r.probe[it, 1, chunk_rows(m, q), :]
            for s in range(4):
                o_re = r.patch[j + s, 0, upper]
                o_im = r.patch[j + s, 1, upper]
                cols = slice(s * side, (s + 1) * side)
                ops[upper, cols] = (p_re * o_re - p_im * o_im).astype(BF16)
                ops[lower, cols] = (p_re * o_im + p_im * o_re).astype(BF16)

    def spectra(k, order, mids):
        m, j = quad(k, order)
        all_far = dot(mids[...], r.inv[...])
        for s in range(4):
            far = all_far[s * side : (s + 1) * side]
            r.far[m, j + s] = far
            r.shrink[j + s] += far[:, :side] * far[:, :side] + far[:, side:] * far[:, side:]

    def residuals(k, order, ops):
        m, j = quad(k, order)
        for q in range(side // CHUNK):
            upper = slice(q * CHUNK, (q + 1) * CHUNK)
            lower = slice(side + q * CHUNK, side + (q + 1) * CHUNK)
            for s in range(4):
                cols = slice(s * side, (s + 1) * side)
                scale = r.shrink[j + s, upper]
                far = r.far[m, j + s, upper, :]
                ops[upper, cols] = (far[:, :side] * scale).astype(BF16)
                ops[lower, cols] = (far[:, side:] * scale).astype(BF16)

    def changes(it, k, order, mids):
        m, j = quad(k, order)
        delta = dot(mids[...], r.fwd[...])
        for q in range(side // CHUNK):
            g_re = r.grad[it, 0, chunk_rows(m, q), :]
            g_im = r.grad[it, 1, chunk_rows(m, q), :]
            for s in range(4):
                upper = slice(q * CHUNK, (q + 1) * CHUNK)
                change = delta[s * side + q * CHUNK : s * side + (q + 1) * CHUNK]
                r.delta[m, j + s, upper, :] = change
                c_re, c_im = change[:, :side], change[:, side:]
                o_re = r.patch[j + s, 0, upper]
                o_im = r.patch[j + s, 1, upper]
                g_re = g_re + (o_re * c_re + o_im * c_im)
                g_im = g_im + (o_re * c_im - o_im * c_re)
            r.grad[it, 0, chunk_rows(m, q), :] = g_re
            r.grad[it, 1, chunk_rows(m, q), :] = g_im

    def object_terms(it, start, stop):
        def one(j, carry):
            for q in range(side // CHUNK):
                g_re = jnp.zeros((CHUNK, side), F32)
                g_im = jnp.zeros((CHUNK, side), F32)
                for m in range(plan.modes):
                    rows_q = slice(m * side + q * CHUNK, m * side + (q + 1) * CHUNK)
                    p_re = r.probe[it, 0, rows_q, :]
                    p_im = r.probe[it, 1, rows_q, :]
                    change = r.delta[m, j, q * CHUNK : (q + 1) * CHUNK, :]
                    c_re, c_im = change[:, :side], change[:, side:]
                    g_re = g_re + (p_re * c_re + p_im * c_im)
                    g_im = g_im + (p_re * c_im - p_im * c_re)
                r.spread[j, 0, tile + q * CHUNK : tile + (q + 1) * CHUNK] = g_re
                r.spread[j, 1, tile + q * CHUNK : tile + (q + 1) * CHUNK] = g_im
            return carry

        lax.fori_loop(start, stop, one, 0)

    bodies = plan.steps * plan.step_bodies
    turns = bodies // 3
    assert bodies % 3 == 0

    def turn_of(step):
        return max(0, -((4 - step * plan.step_bodies) // 3))

    def turn_after(step):
        return -(-((step + 1) * plan.step_bodies) // 3)

    def pipelined(first, second, third, hooks):
        def most(k):
            third(k, r.mids0)
            second(r.ops1, r.mids1)
            first(k + 2, r.ops2)
            third(k + 1, r.mids1)
            second(r.ops2, r.mids2)

        def turn(i, carry):
            for at, acts in sorted(hooks.items()):
                if at < turns - 1:

                    @pl.when(i == at)
                    def _():
                        for act in acts:
                            act()

            k = 3 * i
            most(k)
            first(k + 3, r.ops0)
            third(k + 2, r.mids2)
            second(r.ops0, r.mids0)
            first(k + 4, r.ops1)
            return carry

        first(0, r.ops0)
        second(r.ops0, r.mids0)
        first(1, r.ops1)
        lax.fori_loop(0, turns - 1, turn, 0)
        for act in hooks.get(turns - 1, ()):
            act()
        most(bodies - 3)
        third(bodies - 1, r.mids2)
        for act in hooks.get(turns, ()):
            act()

    def forward(it, order, hooks):
        def first(k, ops):
            waves(it, k, order, ops)

        def second(ops, mids):
            half_way(r.fwd, ops, mids)

        def third(k, mids):
            spectra(k, order, mids)

        pipelined(first, second, third, hooks)

    def backward(it, hooks):
        def shrinks(i, carry):
            for n in range(2):
                j = 2 * i + n
                r.shrink[j] = 1.0 - r.amp[j] / jnp.sqrt(r.shrink[j] + SOFT_FLOOR)
            return carry

        lax.fori_loop(0, plan.count // 2, shrinks, 0)

        def first(k, ops):
            residuals(k, in_turn, ops)

        def second(ops, mids):
            half_way(r.inv, ops, mids)

        def third(k, mids):
            changes(it, k, in_turn, mids)

        pipelined(first, second, third, hooks)

    def in_turn(t):
        return t

    class Hooks(dict):
        def put(self, at, act, *rest):
            self.setdefault(min(max(at, 0), turns), []).append(functools.partial(act, *rest))

    last = plan.steps - 1

    def each(act, it, step):
        for b in blocks_of(step):
            act(it, b)

    def forward_hooks(it, order):
        hooks = Hooks()
        for t in range(1, plan.steps):
            need = turn_of(t)
            hooks.put(need - 1, each, pass_cores, it, order(t))
            hooks.put(need, each, got_cores, it, order(t))
        for w in range(plan.weights):
            hooks.put(turns // 3, reduce_b, weights, it, w)
            hooks.put(turns - 2, reduce_weights, it, w)
        return hooks

    def backward_hooks(it):
        hooks = Hooks()
        for t in range(plan.steps):
            for b in blocks_of(t):
                hooks.put(turn_after(t), reduce_a, grads, it, b)
                if t < last:
                    hooks.put(turn_after(t + 1), reduce_b, grads, it, b)
        hooks.put(turns // 2, settle_weights, it)
        return hooks

    def late_sums(it):
        object_terms(it, 0, plan.count // 2)
        for b in blocks_of(last):
            reduce_b(grads, it, b)
        for t in range(plan.steps - 3):
            each(to_owner, it, t)
        object_terms(it, plan.count // 2, plan.count)
        if last >= 2:
            each(to_owner, it, last - 2)
        fold_object(it)
        for t in range(max(0, last - 1), plan.steps):
            each(to_owner, it, t)

    send_object(0)
    spread_rows(0, gy)
    spread_chips(0, gy)
    if plan.step_blocks > 1:
        each(pass_chips, 0, first_order(0))
    each(pass_cores, 0, first_order(0))
    from_neighbours(0, r.halo, r.halo_sem)
    widen(0)
    cut_patches(0)
    for t in range(1, plan.steps):
        each(pass_chips, 0, first_order(t))
    for w in range(plan.weights):
        reduce_a(weights, 0, w)
    for copy in loads[1:]:
        copy.wait()
    each(got_cores, 0, first_order(0))
    forward(0, first_order, forward_hooks(0, first_order))
    fold_weights(0)
    loads[0].wait()
    backward(0, backward_hooks(0))
    late_sums(0)
    for t in range(max(0, last - 1)):
        for b in blocks_of(t):
            renew(b)
    r.obj[1] = new_object(0)
    send_object(1)
    for t in range(max(0, last - 1), plan.steps):
        for b in blocks_of(t):
            renew(b)
    for t in range(max(0, last - 1)):
        each(pass_chips, 1, t)
    from_neighbours(1, r.halo, r.halo_sem)
    widen(1)
    cut_patches(1)
    each(pass_cores, 1, 0)
    for t in range(max(0, last - 1), plan.steps):
        each(pass_chips, 1, t)
    for w in range(plan.weights):
        reduce_a(weights, 1, w)
    each(got_cores, 1, 0)
    forward(1, in_turn, forward_hooks(1, in_turn))
    fold_weights(1)
    backward(1, backward_hooks(1))
    late_sums(1)
    final = new_object(1)
    object_out[0] = final[:, :tile]
    object_out[1] = half_turn(final)[:, :tile]
    new = owned(1, gy)
    for plane in range(2):
        if plan.split:
            probe_out[plane] = new[plane]
        else:
            probe_out[plane] = jnp.where(core == 0, new[plane][: plan.own], new[plane][plan.own :])

    for it in range(ITERS):
        sent_to_neighbours(it, r.halo, r.halo_sem)
        sent_to_neighbours(it, r.fold_rx, r.fold_sem)
        sent_to_neighbours(it, r.wfold_rx, r.wfold_sem)
        for ch, blocks in ((grads, plan.gy), (weights, plan.weights)):
            for b in range(blocks):
                await_bytes(ch.rx_a.at[it, b], ch.a_sem.at[0, it, b])
                await_bytes(ch.rx_b.at[it, b], ch.b_sem.at[0, it, b])
        for w in range(plan.weights):
            await_bytes(weights.rx_c.at[it, w], weights.c_sem.at[0, it, w])
        for b in range(plan.gy):

            @pl.when(gy != b)
            def _():
                await_bytes(grads.sum_b.at[it, b], grads.c_sem.at[0, it, b])

            await_bytes(probe_span(it, chips - 1), r.gb_sem.at[0, it, b])
            if plan.split:
                await_bytes(probe_span(it, chips), r.ga_sem.at[0, it, b])
        await_bytes(probe_span(it, ny - 1), r.row_sem.at[it, ny])


def table(side):
    index = np.arange(side, dtype=np.int32)
    angles = (index[:, None] * index[None, :] % side).astype(np.float32) * np.float32(2.0 * math.pi / side)
    factor = np.float32(1.0 / math.sqrt(side))
    cosine, sine = np.cos(angles) * factor, np.sin(angles) * factor
    forward = np.block([[cosine, sine], [-sine, cosine]])
    return jnp.asarray(forward, BF16), jnp.asarray(forward.T, BF16)


def solution(mesh):
    def whole(object_field, probe_modes, positions, amplitudes):
        plan = Plan(mesh, object_field, probe_modes, positions, amplitudes)
        scratch = plan.scratch()

        def local(object_tile, own, places, measured):
            if not plan.split:
                groups = [[2 * i, 2 * i + 1] for i in range(plan.chips)]
                own = lax.all_gather(own, "gx", axis_index_groups=groups, axis=1, tiled=True)
            forward, inverse = table(plan.side)
            vmem = pl.BlockSpec(memory_space=pltpu.VMEM)
            hbm = pl.BlockSpec(memory_space=pl.ANY)
            return pl.pallas_call(
                functools.partial(program, plan, tuple(scratch)),
                out_shape=(
                    jax.ShapeDtypeStruct(object_tile.shape, F32),
                    jax.ShapeDtypeStruct((2, plan.own, plan.side), F32),
                ),
                in_specs=[pl.BlockSpec(memory_space=pltpu.SMEM), vmem, vmem, hbm, hbm, hbm],
                out_specs=(vmem, vmem),
                scratch_shapes=list(scratch.values()),
                compiler_params=pltpu.CompilerParams(
                    collective_id=0, has_side_effects=True, vmem_limit_bytes=56 * 1024 * 1024
                ),
                name="iterations",
            )(
                places.reshape(-1, 2),
                object_tile,
                own,
                measured.reshape(-1, plan.side, plan.side),
                forward,
                inverse,
            )

        return jax.shard_map(
            local,
            mesh=mesh,
            in_specs=(
                P(None, "gy", "gx"),
                P(None, ("gy", "gx"), None),
                P("gy", "gx", None, None),
                P("gy", "gx", None, None, None),
            ),
            out_specs=(P(None, "gy", "gx"), P(None, ("gy", "gx"), None)),
            check_vma=False,
        )(object_field, probe_modes, positions, amplitudes)

    return whole
```
